512 devices in a mesh: row: 16 (over y, core), col: 32 (over z, x).
Axes of the slice: x: 4, y: 8, z: 8, core: 2. Of those that a mesh axis runs over, the one named last changes fastest.
Arguments:
- templates: float32 [1536, 3, 1024], P(('row', 'col')), may hold values from -600 to 600
Outputs:
- similar: float32 [1536, 1536], P(('row', 'col'))
The draws below stay inside these ranges and needn't reach their ends.
All inputs are finite; a program needn't handle non-finite values.
Results may differ from the reference program's by a relative error of at most 0.0012.
Values may be sent and summed in bfloat16 or wider, within the bound.
No kernel may reach another device: no remote copies, remote signals or barrier semaphores. Data moves between devices by JAX's collectives and lax.ppermute only.
A program may use at most 128 MiB of HBM per device.

```python
import math
import jax
import jax.numpy as jnp
from jax import lax

COMP = 3
SAMPLES = 1024
LAGS = 512
NFFT = 1280
NT = 1536


def draw_templates(key, part):
    subkeys = jax.random.split(key, 6)
    noise_part = jnp.clip(jax.random.normal(subkeys[0], (NT, COMP, SAMPLES), jnp.float32), -6.0, 6.0)
    weight = jax.random.uniform(subkeys[4], (NT, 1, 1), jnp.float32, 0.0, 1.5)
    scales = jnp.exp(jax.random.uniform(subkeys[5], (NT, COMP, 1), jnp.float32, 0.0, jnp.log(10.0)))
    clusters = jnp.clip(jax.random.normal(subkeys[1], (8, COMP, SAMPLES), jnp.float32), -6.0, 6.0)
    member = jax.random.randint(subkeys[2], (NT,), 0, 8)
    shifts = jax.random.randint(subkeys[3], (NT,), -(LAGS // 4), LAGS // 4 + 1)
    source_idx = (jnp.arange(SAMPLES, dtype=jnp.int32)[None, :] - shifts[:, None]) % SAMPLES
    chosen = clusters[member]
    shifted = jnp.take_along_axis(chosen, jnp.broadcast_to(source_idx[:, None, :], (NT, COMP, SAMPLES)), axis=2)
    return ((weight * shifted + noise_part) * scales).astype(jnp.float32)


def setup_inputs(seed: int = 0) -> dict:
    splits = jax.random.split(jax.random.key(seed), 2)
    templates = draw_templates(jax.random.fold_in(splits[1], 71), 0)
    return {"templates": templates}


def normalize(templates):
    scaling = lax.rsqrt(lax.optimization_barrier(jnp.mean(templates * templates, axis=2, keepdims=True)) + 1e-06) / math.sqrt(templates.shape[2])
    return (templates * scaling).astype(jnp.bfloat16)

def forward_table(samples, transform_len):
    half_len = transform_len // 2
    sample_idx = jnp.arange(samples, dtype=jnp.int32)[:, None]
    slot_idx = jnp.arange(transform_len, dtype=jnp.int32)[None, :]
    freq_idx = jnp.where(slot_idx < half_len, slot_idx, slot_idx - half_len)
    phases = sample_idx * freq_idx % transform_len
    angles = phases.astype(jnp.float32) * (2.0 * math.pi / transform_len)
    nyquist = jnp.where(sample_idx % 2 == 0, 1.0, -1.0)
    basis = jnp.where(slot_idx < half_len, jnp.cos(angles), jnp.where(slot_idx == half_len, nyquist, -jnp.sin(angles)))
    return basis.astype(jnp.bfloat16)

def inverse_table(transform_len, lag_total):
    half_len = transform_len // 2
    slot_idx = jnp.arange(transform_len, dtype=jnp.int32)[:, None]
    lag_idx = jnp.arange(lag_total, dtype=jnp.int32)[None, :] - lag_total // 2
    freq_idx = jnp.where(slot_idx < half_len, slot_idx, slot_idx - half_len)
    phases = freq_idx * lag_idx % transform_len
    angles = phases.astype(jnp.float32) * (2.0 * math.pi / transform_len)
    weight = jnp.where(freq_idx == 0, 1.0, 2.0) / transform_len
    nyquist = jnp.where(lag_idx % 2 == 0, 1.0, -1.0) / transform_len
    basis = jnp.where(slot_idx < half_len, weight * jnp.cos(angles), jnp.where(slot_idx == half_len, nyquist, -weight * jnp.sin(angles)))
    return basis.astype(jnp.bfloat16)

def spectra_of(normed, basis):
    row_total, comps, samples = normed.shape
    flattened = normed.reshape(row_total * comps, samples)
    spectrum = jnp.dot(flattened, basis, preferred_element_type=jnp.float32)
    return spectrum.astype(jnp.bfloat16).reshape(row_total, comps, basis.shape[1])

def pair_einsum(left_part, right_part):
    return jnp.einsum('icf,jcf->ijf', left_part.astype(jnp.float32), right_part.astype(jnp.float32))

def similarity(left_spec, right_spec, inverse):
    half_len = left_spec.shape[2] // 2
    left_real = left_spec[:, :, :half_len]
    left_imag = left_spec[:, :, half_len:]
    right_real = right_spec[:, :, :half_len]
    right_imag = right_spec[:, :, half_len:]
    above_zero = jnp.arange(half_len, dtype=jnp.int32) >= 1
    right_masked = jnp.where(above_zero, right_imag, jnp.zeros_like(right_imag))
    left_masked = jnp.where(above_zero, left_real, jnp.zeros_like(left_real))
    right_turned = jnp.where(above_zero, -right_real, right_imag)
    even_part = pair_einsum(jnp.concatenate([left_real, left_imag], axis=1), jnp.concatenate([right_real, right_masked], axis=1))
    odd_part = pair_einsum(jnp.concatenate([left_masked, left_imag], axis=1), jnp.concatenate([right_imag, right_turned], axis=1))
    cross_spec = jnp.concatenate([even_part, odd_part], axis=2).astype(jnp.bfloat16)
    left_rows = left_spec.shape[0]
    right_rows = right_spec.shape[0]
    lagged = jnp.dot(cross_spec.reshape(left_rows * right_rows, 2 * half_len), inverse, preferred_element_type=jnp.float32)
    return lax.optimization_barrier(jnp.max(lagged, axis=1)).reshape(left_rows, right_rows)

def reference(templates):
    forward = forward_table(SAMPLES, NFFT)
    inverse = inverse_table(NFFT, LAGS)
    spectrum = spectra_of(normalize(templates), forward)
    block_total = math.gcd(NT, 64)
    pieces = spectrum.reshape(block_total, NT // block_total, COMP, NFFT)
    similar = lax.map(lambda row_piece: similarity(row_piece, spectrum, inverse), pieces)
    return similar.reshape(NT, NT)
```

```python
import functools
import math

import jax
import jax.numpy as jnp
import numpy as np
from jax import lax
from jax.experimental import pallas as pl
from jax.experimental.pallas import tpu as pltpu
from jax.sharding import PartitionSpec as P

LAGS = 512
LANES = 128


def forward_table(samples, transform_len):
    half_len = transform_len // 2
    sample_idx = np.arange(samples)[:, None]
    slot_idx = np.arange(transform_len)[None, :]
    freq_idx = np.where(slot_idx < half_len, slot_idx, slot_idx - half_len)
    phases = (sample_idx * freq_idx) % transform_len
    angles = phases * (2.0 * math.pi / transform_len)
    nyquist = np.where(sample_idx % 2 == 0, 1.0, -1.0)
    basis = np.where(
        slot_idx < half_len,
        np.cos(angles),
        np.where(slot_idx == half_len, nyquist, -np.sin(angles)),
    )
    return basis.astype(np.float32).astype(jnp.bfloat16)


def lag_tables(transform_len, half_lags):
    half_len = transform_len // 2
    freq_idx = np.arange(half_len)[:, None]
    lag_idx = np.concatenate([np.arange(0, half_lags, 2), np.arange(1, half_lags, 2)])[None, :]
    phases = (freq_idx * lag_idx) % transform_len
    angles = phases * (2.0 * math.pi / transform_len)
    weight = np.where(freq_idx == 0, 1.0, 2.0) / transform_len
    even = (weight * np.cos(angles)).astype(np.float32)
    odd = np.where(freq_idx == 0, 0.0, -weight * np.sin(angles)).astype(np.float32)
    return even.astype(jnp.bfloat16), odd.astype(jnp.bfloat16)


def normalize_kernel(copies, x_ref, one_ref, many_ref, rows_ref):
    per_device, comps, samples = x_ref.shape
    parts = samples // LANES
    for t in range(per_device):
        x = x_ref[t]
        scaling = lax.rsqrt(jnp.sum(x * x, axis=1, keepdims=True) / samples + 1e-06) / math.sqrt(samples)
        y = x * scaling
        for a in range(parts):
            rows_ref[pl.ds(t * comps * parts + a, comps, stride=parts), :] = y[:, a * LANES : (a + 1) * LANES]
    packed = rows_ref[...].astype(jnp.bfloat16)
    one_ref[...] = packed
    for q in range(copies):
        many_ref[q] = packed


def normalize(templates, copies):
    per_device, comps, samples = templates.shape
    rows = per_device * comps * samples // LANES
    return pl.pallas_call(
        functools.partial(normalize_kernel, copies),
        out_shape=(
            jax.ShapeDtypeStruct((rows, LANES), jnp.bfloat16),
            jax.ShapeDtypeStruct((copies, rows, LANES), jnp.bfloat16),
        ),
        scratch_shapes=[pltpu.VMEM((rows, LANES), jnp.float32)],
        compiler_params=pltpu.CompilerParams(vmem_limit_bytes=8 << 20),
        name="normalize",
    )(templates)


def similarity_kernel(
    comps, samples, chunk, step, *refs
):
    (left_ref, right_ref, basis_ref, even_ref, odd_ref, out_ref,
     rows_ref, lw_ref, rw_ref, lr_ref, li_ref, ls_ref, rr_ref, ri_ref, rd_ref,
     ce0, co0, ce1, co1, me_ref, mo_ref) = refs
    parts = samples // LANES
    left = left_ref.shape[0] // (comps * parts)
    right = right_ref.shape[0] // (comps * parts)
    half_len = even_ref.shape[0]
    tiles = half_len // LANES

    def waves(src_ref, wave_ref, count):
        total = count * comps * parts
        rows_ref[0:total, :] = src_ref[...].astype(jnp.float32)
        for c in range(comps):
            for a in range(parts):
                wave_ref[c * count : (c + 1) * count, a * LANES : (a + 1) * LANES] = rows_ref[
                    pl.ds(c * parts + a, count, stride=comps * parts), :
                ].astype(jnp.bfloat16)

    waves(left_ref, lw_ref, left)
    waves(right_ref, rw_ref, right)

    def spectrum(wave_ref):
        return jnp.dot(wave_ref[...], basis_ref[...], preferred_element_type=jnp.float32)

    first = lax.broadcasted_iota(jnp.int32, (1, half_len), 1) == 0

    def split(spec):
        rounded = spec.astype(jnp.bfloat16).astype(jnp.float32)
        slots = rounded[:, half_len:]
        top = jnp.where(first[:, :LANES], slots[:, :LANES], 0.0)
        return rounded[:, :half_len], jnp.where(first, 0.0, slots), top

    real, imag, top_left = split(spectrum(lw_ref))
    for f in range(tiles):
        fs = slice(f * LANES, (f + 1) * LANES)
        lr_ref[f] = real[:, fs]
        li_ref[f] = imag[:, fs]
        ls_ref[f] = real[:, fs] + imag[:, fs]
    real, imag, top_right = split(spectrum(rw_ref))
    rr_ref[...] = real
    ri_ref[...] = imag
    rd_ref[...] = imag - real

    nt = (((1,), (1,)), ((), ()))
    shift = LAGS // 2
    highest = jnp.zeros((right, left), jnp.float32)
    earliest = jnp.zeros((right, left), jnp.float32)
    for c in range(comps):
        lsl, rsl = slice(c * left, (c + 1) * left), slice(c * right, (c + 1) * right)
        highest += lax.dot_general(
            top_right[rsl].astype(jnp.bfloat16), top_left[lsl].astype(jnp.bfloat16), nt,
            preferred_element_type=jnp.float32,
        )
        earliest += lax.dot_general(
            rw_ref[rsl, : samples - shift], lw_ref[lsl, shift:], nt,
            preferred_element_type=jnp.float32,
        )

    def cross(index, even_out, odd_out):
        for f in range(tiles):
            fs = slice(f * LANES, (f + 1) * LANES)
            for u in range(chunk):
                i = index * chunk + u
                lr = [lr_ref[f, pl.ds(c * left + i, 1), :] for c in range(comps)]
                li = [li_ref[f, pl.ds(c * left + i, 1), :] for c in range(comps)]
                ls = [ls_ref[f, pl.ds(c * left + i, 1), :] for c in range(comps)]
                for j in range(0, right, step):
                    rr = rr_ref[j : j + step, fs] * lr[0]
                    ii = ri_ref[j : j + step, fs] * li[0]
                    mm = rd_ref[j : j + step, fs] * ls[0]
                    for c in range(1, comps):
                        rows = slice(c * right + j, c * right + j + step)
                        rr += rr_ref[rows, fs] * lr[c]
                        ii += ri_ref[rows, fs] * li[c]
                        mm += rd_ref[rows, fs] * ls[c]
                    rows = slice(u * right + j, u * right + j + step)
                    even_out[rows, fs] = (rr + ii).astype(jnp.bfloat16)
                    odd_out[rows, fs] = (mm + (rr - ii)).astype(jnp.bfloat16)

    column = lax.broadcasted_iota(jnp.int32, (1, left), 1)

    def lags(index, even_in, odd_in):
        even = jnp.dot(even_in[...], even_ref[...], preferred_element_type=jnp.float32)
        odd = jnp.dot(odd_in[...], odd_ref[...], preferred_element_type=jnp.float32)
        best = even + jnp.abs(odd)
        for u in range(chunk):
            here = column == index * chunk + u
            rows = best[u * right : (u + 1) * right]
            me_ref[...] = jnp.where(here, jnp.max(rows[:, :LANES], axis=1, keepdims=True), me_ref[...])
            mo_ref[...] = jnp.where(here, jnp.max(rows[:, LANES:], axis=1, keepdims=True), mo_ref[...])

    me_ref[...] = jnp.zeros_like(me_ref)
    mo_ref[...] = jnp.zeros_like(mo_ref)
    count = left // chunk
    cross(0, ce0, co0)

    def both(n, carry):
        cross(2 * n + 1, ce1, co1)
        lags(2 * n, ce0, co0)
        cross(jnp.minimum(2 * n + 2, count - 1), ce0, co0)
        lags(2 * n + 1, ce1, co1)
        return carry

    lax.fori_loop(0, count // 2, both, 0)

    alternating = highest.astype(jnp.bfloat16).astype(jnp.float32) / (2 * half_len)
    best = jnp.maximum(me_ref[...] + alternating, mo_ref[...] - alternating)
    best = jnp.maximum(best, earliest)
    wide = jnp.concatenate([best, jnp.zeros((right, LANES - left), jnp.float32)], axis=1)
    tall = jnp.concatenate([wide, jnp.zeros((LANES - right, LANES), jnp.float32)], axis=0)
    turned = tall.T
    owners, per_owner = out_ref.shape[0], left // out_ref.shape[0]
    for r in range(owners):
        out_ref[r, 0:per_owner, :] = turned[r * per_owner : (r + 1) * per_owner, :]


def similarity(left_waves, right_waves, comps, samples, owners):
    transform_len = samples + LAGS // 2
    half_len = transform_len // 2
    parts = samples // LANES
    left = left_waves.shape[0] // (comps * parts)
    right = right_waves.shape[0] // (comps * parts)
    basis = jnp.asarray(forward_table(samples, transform_len))
    even, odd = (jnp.asarray(t) for t in lag_tables(transform_len, LAGS // 2))
    chunk, step = 2, 32
    f32, bf16 = jnp.float32, jnp.bfloat16
    return pl.pallas_call(
        functools.partial(similarity_kernel, comps, samples, chunk, step),
        out_shape=jax.ShapeDtypeStruct((owners, 8, LANES), f32),
        scratch_shapes=[
            pltpu.VMEM((right * comps * parts, LANES), f32),
            pltpu.VMEM((left * comps, samples), bf16),
            pltpu.VMEM((right * comps, samples), bf16),
            *[pltpu.VMEM((half_len // LANES, left * comps, LANES), f32)] * 3,
            *[pltpu.VMEM((right * comps, half_len), f32)] * 3,
            *[pltpu.VMEM((chunk * right, half_len), bf16)] * 4,
            *[pltpu.VMEM((right, left), f32)] * 2,
        ],
        compiler_params=pltpu.CompilerParams(vmem_limit_bytes=28 << 20),
        cost_estimate=pl.CostEstimate(flops=8_000_000_000, bytes_accessed=4_000_000, transcendentals=0),
        name="similarity",
    )(left_waves, right_waves, basis, even, odd)


def assemble_kernel(width, in_ref, out_ref):
    for r in range(in_ref.shape[0]):
        out_ref[:, r * width : (r + 1) * width] = in_ref[r, 0 : out_ref.shape[0], 0:width]


def body(templates):
    per_device, comps, samples = templates.shape
    row_count = lax.axis_size("row")
    col_count = lax.axis_size("col")
    one, many = normalize(templates, col_count)
    partners = lax.all_to_all(many, "col", split_axis=0, concat_axis=0, tiled=True)
    owned = lax.all_gather(one, "row", tiled=True)
    partners = partners.reshape(col_count * one.shape[0], LANES)
    block = similarity(owned, partners, comps, samples, row_count)
    mine = lax.all_to_all(block, "row", split_axis=0, concat_axis=0, tiled=True)
    width = col_count * per_device
    return pl.pallas_call(
        functools.partial(assemble_kernel, width),
        out_shape=jax.ShapeDtypeStruct((per_device, row_count * width), jnp.float32),
        name="assemble",
    )(mine)


def solution(mesh):
    placed = (P(("row", "col"), None, None),)
    return jax.shard_map(
        body, mesh=mesh, in_specs=placed, out_specs=P(("row", "col"), None), check_vma=False
    )
```

```python
import functools
import math

import jax
import jax.numpy as jnp
import numpy as np
from jax import lax
from jax.experimental import pallas as pl
from jax.experimental.pallas import tpu as pltpu
from jax.sharding import PartitionSpec as P

LAGS = 512
LANES = 128


def frequency_order(half_len):
    quarter, whole = half_len // 2, half_len // 2 // LANES * LANES
    even, odd = 2 * np.arange(quarter), 2 * np.arange(quarter) + 1
    return np.concatenate([even[:whole], even[whole:], odd[whole:], odd[:whole]])


def transform_tables(transform_len, half_lags):
    half_len = transform_len // 2
    step = 2.0 * math.pi / transform_len
    order = frequency_order(half_len)
    whole = half_len // 2 // LANES * LANES
    rest = half_len // 2 - whole
    sample = np.arange(half_len)[:, None]
    angles = (sample * order[None, :]) % transform_len * step
    real = np.cos(angles)
    imag = np.where(order[None, :] == 0, np.where(sample % 2 == 0, 1.0, -1.0), -np.sin(angles))
    evens, evens_rest = slice(0, whole), slice(whole, whole + rest)
    odds_rest, odds = slice(whole + rest, half_len - whole), slice(half_len - whole, half_len)
    forward = [real[:, evens], imag[:, evens], real[:, evens_rest], imag[:, evens_rest]]
    forward += [real[:, odds], imag[:, odds], real[:, odds_rest], imag[:, odds_rest]]
    lag = np.concatenate([np.arange(0, half_lags, 2), np.arange(1, half_lags, 2)])[None, :]
    angles = (order[:, None] * lag) % transform_len * step
    weight = np.where(order[:, None] == 0, 1.0, 2.0) / transform_len
    cosine = weight * np.cos(angles)
    sine = np.where(order[:, None] == 0, 0.0, -weight * np.sin(angles))
    return np.concatenate([*forward, cosine, sine], axis=1).astype(np.float32).astype(jnp.bfloat16)


def normalize_kernel(copies, x_ref, one_ref, many_ref, rows_ref):
    per_device, comps, samples = x_ref.shape
    parts = samples // LANES
    for t in range(per_device):
        x = x_ref[t]
        scaling = lax.rsqrt(jnp.sum(x * x, axis=1, keepdims=True) / samples + 1e-06) / math.sqrt(samples)
        y = x * scaling
        for a in range(parts):
            rows_ref[pl.ds(t * comps * parts + a, comps, stride=parts), :] = y[:, a * LANES : (a + 1) * LANES]
    packed = rows_ref[...].astype(jnp.bfloat16)
    one_ref[...] = packed
    for q in range(copies):
        many_ref[q] = packed


def normalize(templates, copies):
    per_device, comps, samples = templates.shape
    rows = per_device * comps * samples // LANES
    return pl.pallas_call(
        functools.partial(normalize_kernel, copies),
        out_shape=(
            jax.ShapeDtypeStruct((rows, LANES), jnp.bfloat16),
            jax.ShapeDtypeStruct((copies, rows, LANES), jnp.bfloat16),
        ),
        scratch_shapes=[pltpu.VMEM((rows, LANES), jnp.float32)],
        compiler_params=pltpu.CompilerParams(vmem_limit_bytes=8 << 20),
        name="normalize",
    )(templates)


def similarity_kernel(comps, samples, chunk, step, *refs):
    (left_ref, right_ref, tables_hbm, out_ref,
     basis_ref, even_ref, odd_ref, rows_ref, wave_ref,
     l1_ref, l2_ref, l3_ref, r1_ref, r2_ref, r3_ref,
     ce0, co0, ce1, co1, me_ref, mo_ref, sems) = refs
    parts = samples // LANES
    left = left_ref.shape[0] // (comps * parts)
    right = right_ref.shape[0] // (comps * parts)
    half_len, lag_count = even_ref.shape
    tiles = half_len // LANES

    width = 2 * half_len
    sources = [slice(0, width), slice(width, width + lag_count), slice(width + lag_count, width + 2 * lag_count)]
    copies = [
        pltpu.make_async_copy(tables_hbm.at[:, source], target, sems.at[k])
        for k, (source, target) in enumerate(zip(sources, (basis_ref, even_ref, odd_ref)))
    ]
    for copy in copies:
        copy.start()

    def waves(src_ref, base, count):
        total = count * comps * parts
        rows_ref[0:total, :] = src_ref[...].astype(jnp.float32)
        for c in range(comps):
            for a in range(parts):
                wave_ref[base + c * count : base + (c + 1) * count, a * LANES : (a + 1) * LANES] = rows_ref[
                    pl.ds(c * parts + a, count, stride=comps * parts), :
                ].astype(jnp.bfloat16)

    split = comps * left
    waves(left_ref, 0, left)
    waves(right_ref, split, right)

    nt = (((1,), (1,)), ((), ()))
    shift = LAGS // 2
    earliest = jnp.zeros((right, left), jnp.float32)
    for c in range(comps):
        earliest += lax.dot_general(
            wave_ref[split + c * right : split + (c + 1) * right, : samples - shift],
            wave_ref[c * left : (c + 1) * left, shift:],
            nt, preferred_element_type=jnp.float32,
        )

    copies[0].wait()
    tail = samples - half_len

    def product(cols):
        low = jnp.dot(wave_ref[:, :half_len], basis_ref[:, cols], preferred_element_type=jnp.float32)
        high = jnp.dot(wave_ref[:, half_len:], basis_ref[:tail, cols], preferred_element_type=jnp.float32)
        return low, high

    def rounded(values):
        return values.astype(jnp.bfloat16).astype(jnp.float32)

    low, high = product(slice(0, half_len))
    evens = rounded(low + high)
    low, high = product(slice(half_len, width))
    odds = rounded(low - high)
    whole = half_len // 2 // LANES
    lane = lax.broadcasted_iota(jnp.int32, (1, LANES), 1)

    def tile(values, k):
        return values[:, k * LANES : (k + 1) * LANES]

    def parts_of(f):
        if f < whole:
            return tile(evens, f), tile(evens, whole + f)
        if f > whole:
            return tile(odds, f - whole - 1), tile(odds, f - 1)
        a, b = tile(evens, 2 * whole), tile(odds, 2 * whole)
        half = LANES // 2
        return (
            jnp.where(lane < half, a, pltpu.roll(b, half, 1)),
            jnp.where(lane < half, pltpu.roll(a, half, 1), b),
        )

    top = None
    for f in range(tiles):
        fs = slice(f * LANES, (f + 1) * LANES)
        real, imag = parts_of(f)
        if f == 0:
            top = jnp.where(lane == 0, imag, 0.0).astype(jnp.bfloat16)
            imag = jnp.where(lane == 0, 0.0, imag)
        l1_ref[f] = real[:split]
        l2_ref[f] = real[:split] - imag[:split]
        l3_ref[f] = real[:split] + imag[:split]
        r1_ref[:, fs] = real[split:] + imag[split:]
        r2_ref[:, fs] = imag[split:]
        r3_ref[:, fs] = real[split:]
    highest = jnp.zeros((right, left), jnp.float32)
    for c in range(comps):
        highest += lax.dot_general(
            top[split + c * right : split + (c + 1) * right], top[c * left : (c + 1) * left],
            nt, preferred_element_type=jnp.float32,
        )

    def cross(index, even_out, odd_out):
        for f in range(tiles):
            fs = slice(f * LANES, (f + 1) * LANES)
            for u in range(chunk):
                i = index * chunk + u
                l1 = [l1_ref[f, pl.ds(c * left + i, 1), :] for c in range(comps)]
                l2 = [l2_ref[f, pl.ds(c * left + i, 1), :] for c in range(comps)]
                l3 = [l3_ref[f, pl.ds(c * left + i, 1), :] for c in range(comps)]
                for j in range(0, right, step):
                    k1 = r1_ref[j : j + step, fs] * l1[0]
                    k2 = r2_ref[j : j + step, fs] * l2[0]
                    k3 = r3_ref[j : j + step, fs] * l3[0]
                    for c in range(1, comps):
                        rows = slice(c * right + j, c * right + j + step)
                        k1 += r1_ref[rows, fs] * l1[c]
                        k2 += r2_ref[rows, fs] * l2[c]
                        k3 += r3_ref[rows, fs] * l3[c]
                    rows = slice(u * right + j, u * right + j + step)
                    even_out[rows, fs] = (k1 - k2).astype(jnp.bfloat16)
                    odd_out[rows, fs] = (k1 - k3).astype(jnp.bfloat16)

    column = lax.broadcasted_iota(jnp.int32, (1, left), 1)

    def lags(index, even_in, odd_in):
        even = jnp.dot(even_in[...], even_ref[...], preferred_element_type=jnp.float32)
        odd = jnp.dot(odd_in[...], odd_ref[...], preferred_element_type=jnp.float32)
        best = even + jnp.abs(odd)
        for u in range(chunk):
            here = column == index * chunk + u
            rows = best[u * right : (u + 1) * right]
            me_ref[...] = jnp.where(here, jnp.max(rows[:, :LANES], axis=1, keepdims=True), me_ref[...])
            mo_ref[...] = jnp.where(here, jnp.max(rows[:, LANES:], axis=1, keepdims=True), mo_ref[...])

    me_ref[...] = jnp.zeros_like(me_ref)
    mo_ref[...] = jnp.zeros_like(mo_ref)
    count = left // chunk
    cross(0, ce0, co0)
    copies[1].wait()
    copies[2].wait()

    def both(n, carry):
        cross(2 * n + 1, ce1, co1)
        lags(2 * n, ce0, co0)
        cross(jnp.minimum(2 * n + 2, count - 1), ce0, co0)
        lags(2 * n + 1, ce1, co1)
        return carry

    lax.fori_loop(0, count // 2, both, 0)

    alternating = highest.astype(jnp.bfloat16).astype(jnp.float32) / (2 * half_len)
    best = jnp.maximum(me_ref[...] + alternating, mo_ref[...] - alternating)
    best = jnp.maximum(best, earliest)
    wide = jnp.concatenate([best, jnp.zeros((right, LANES - left), jnp.float32)], axis=1)
    tall = jnp.concatenate([wide, jnp.zeros((LANES - right, LANES), jnp.float32)], axis=0)
    turned = tall.T
    owners, per_owner = out_ref.shape[0], left // out_ref.shape[0]
    for r in range(owners):
        out_ref[r, 0:per_owner, :] = turned[r * per_owner : (r + 1) * per_owner, :]


def similarity(left_waves, right_waves, comps, samples, owners):
    transform_len = samples + LAGS // 2
    half_len = transform_len // 2
    parts = samples // LANES
    left = left_waves.shape[0] // (comps * parts)
    right = right_waves.shape[0] // (comps * parts)
    tables = jnp.asarray(transform_tables(transform_len, LAGS // 2))
    chunk, step = 4, 32
    f32, bf16 = jnp.float32, jnp.bfloat16
    return pl.pallas_call(
        functools.partial(similarity_kernel, comps, samples, chunk, step),
        out_shape=jax.ShapeDtypeStruct((owners, 8, LANES), f32),
        in_specs=[pl.BlockSpec(memory_space=pltpu.VMEM)] * 2 + [pl.BlockSpec(memory_space=pltpu.HBM)],
        scratch_shapes=[
            pltpu.VMEM((half_len, transform_len), bf16),
            *[pltpu.VMEM((half_len, LAGS // 2), bf16)] * 2,
            pltpu.VMEM((right * comps * parts, LANES), f32),
            pltpu.VMEM(((left + right) * comps, samples), bf16),
            *[pltpu.VMEM((half_len // LANES, left * comps, LANES), f32)] * 3,
            *[pltpu.VMEM((right * comps, half_len), f32)] * 3,
            *[pltpu.VMEM((chunk * right, half_len), bf16)] * 4,
            *[pltpu.VMEM((right, left), f32)] * 2,
            pltpu.SemaphoreType.DMA((3,)),
        ],
        compiler_params=pltpu.CompilerParams(vmem_limit_bytes=54_500_000),
        cost_estimate=pl.CostEstimate(flops=8_000_000_000, bytes_accessed=4_000_000, transcendentals=0),
        name="similarity",
    )(left_waves, right_waves, tables)


def assemble_kernel(width, in_ref, out_ref):
    for r in range(in_ref.shape[0]):
        out_ref[:, r * width : (r + 1) * width] = in_ref[r, 0 : out_ref.shape[0], 0:width]


def body(templates):
    per_device, comps, samples = templates.shape
    row_count = lax.axis_size("row")
    col_count = lax.axis_size("col")
    one, many = normalize(templates, col_count)
    partners = lax.all_to_all(many, "col", split_axis=0, concat_axis=0, tiled=True)
    owned = lax.all_gather(one, "row", tiled=True)
    partners = partners.reshape(col_count * one.shape[0], LANES)
    block = similarity(owned, partners, comps, samples, row_count)
    mine = lax.all_to_all(block, "row", split_axis=0, concat_axis=0, tiled=True)
    width = col_count * per_device
    return pl.pallas_call(
        functools.partial(assemble_kernel, width),
        out_shape=jax.ShapeDtypeStruct((per_device, row_count * width), jnp.float32),
        compiler_params=pltpu.CompilerParams(vmem_limit_bytes=4 << 20),
        name="assemble",
    )(mine)


def solution(mesh):
    placed = (P(("row", "col"), None, None),)
    return jax.shard_map(
        body, mesh=mesh, in_specs=placed, out_specs=P(("row", "col"), None), check_vma=False
    )
```

```python
import functools
import math

import jax
import jax.numpy as jnp
import numpy as np
from jax import lax
from jax.experimental import pallas as pl
from jax.experimental.pallas import tpu as pltpu
from jax.sharding import PartitionSpec as P

LAGS = 512
LANES = 128


FINE = 32


def transform_tables(samples, transform_len, half_lags):
    half_len = transform_len // 2
    step = 2.0 * math.pi / transform_len
    freq = np.arange(half_len)
    lag = np.concatenate([np.arange(0, half_lags, 2), np.arange(1, half_lags, 2)])[None, :]
    angles = (freq[:, None] * lag) % transform_len * step
    weight = np.where(freq[:, None] == 0, 1.0, 2.0) / transform_len
    inverse = np.zeros((half_len, half_len), np.float32)
    inverse[:, :half_lags] = weight * np.cos(angles)
    inverse[:, half_lags : 2 * half_lags] = np.where(freq[:, None] == 0, 0.0, -weight * np.sin(angles))
    fine = (np.arange(FINE)[:, None] * freq) % transform_len * step
    coarse = (FINE * np.arange(samples // FINE)[:, None] * freq) % transform_len * step
    left = np.concatenate([np.cos(fine), np.sin(fine), np.cos(coarse), -np.sin(coarse)])
    rows = [inverse.astype(jnp.bfloat16)]
    for _ in range(3):
        rows.append(left.astype(np.float32).astype(jnp.bfloat16))
        left = left - rows[-1].astype(np.float64)
    return np.concatenate(rows)


def normalize_kernel(copies, x_ref, one_ref, many_ref, rows_ref):
    per_device, comps, samples = x_ref.shape
    parts = samples // LANES
    for t in range(per_device):
        x = x_ref[t]
        scaling = lax.rsqrt(jnp.sum(x * x, axis=1, keepdims=True) / samples + 1e-06) / math.sqrt(samples)
        y = x * scaling
        for a in range(parts):
            rows_ref[pl.ds(t * comps * parts + a, comps, stride=parts), :] = y[:, a * LANES : (a + 1) * LANES]
    packed = rows_ref[...].astype(jnp.bfloat16)
    one_ref[...] = packed
    for q in range(copies):
        many_ref[q] = packed


def normalize(templates, copies):
    per_device, comps, samples = templates.shape
    rows = per_device * comps * samples // LANES
    return pl.pallas_call(
        functools.partial(normalize_kernel, copies),
        out_shape=(
            jax.ShapeDtypeStruct((rows, LANES), jnp.bfloat16),
            jax.ShapeDtypeStruct((copies, rows, LANES), jnp.bfloat16),
        ),
        scratch_shapes=[pltpu.VMEM((rows, LANES), jnp.float32)],
        compiler_params=pltpu.CompilerParams(vmem_limit_bytes=8 << 20),
        name="normalize",
    )(templates)


def similarity_kernel(comps, samples, chunk, step, *refs):
    (left_ref, right_ref, tables_hbm, out_ref,
     part_ref, factor_ref, basis_ref, even_ref, odd_ref, rows_ref, wave_ref,
     l1_ref, l2_ref, l3_ref, r1_ref, r2_ref, r3_ref,
     ce0, co0, ce1, co1, me_ref, mo_ref, sems) = refs
    parts = samples // LANES
    left = left_ref.shape[0] // (comps * parts)
    right = right_ref.shape[0] // (comps * parts)
    half_len, lag_count = even_ref.shape
    tiles = half_len // LANES

    copies = [
        pltpu.make_async_copy(tables_hbm.at[half_len:, :], part_ref, sems.at[0]),
        pltpu.make_async_copy(tables_hbm.at[:half_len, :lag_count], even_ref, sems.at[1]),
        pltpu.make_async_copy(tables_hbm.at[:half_len, lag_count : 2 * lag_count], odd_ref, sems.at[2]),
    ]
    for copy in copies:
        copy.start()

    def waves(src_ref, base, count):
        total = count * comps * parts
        rows_ref[0:total, :] = src_ref[...].astype(jnp.float32)
        for c in range(comps):
            for a in range(parts):
                wave_ref[base + c * count : base + (c + 1) * count, a * LANES : (a + 1) * LANES] = rows_ref[
                    pl.ds(c * parts + a, count, stride=comps * parts), :
                ].astype(jnp.bfloat16)

    split = comps * left
    waves(left_ref, 0, left)
    waves(right_ref, split, right)

    nt = (((1,), (1,)), ((), ()))
    shift = LAGS // 2
    earliest = jnp.zeros((right, left), jnp.float32)
    for c in range(comps):
        earliest += lax.dot_general(
            wave_ref[split + c * right : split + (c + 1) * right, : samples - shift],
            wave_ref[c * left : (c + 1) * left, shift:],
            nt, preferred_element_type=jnp.float32,
        )

    copies[0].wait()
    count = factor_ref.shape[0]
    factor_ref[...] = (
        part_ref[:count].astype(jnp.float32)
        + part_ref[count : 2 * count].astype(jnp.float32)
        + part_ref[2 * count :].astype(jnp.float32)
    )
    lane = lax.broadcasted_iota(jnp.int32, (FINE, LANES), 1)
    row = lax.broadcasted_iota(jnp.int32, (FINE, LANES), 0)
    alternate = jnp.where(lax.rem(row, 2) == 0, 1.0, -1.0)
    for f in range(tiles):
        fs = slice(f * LANES, (f + 1) * LANES)
        cos_fine, sin_fine = factor_ref[:FINE, fs], factor_ref[FINE : 2 * FINE, fs]
        for a in range(samples // FINE):
            at = 2 * FINE + a
            cos_coarse = factor_ref[at : at + 1, fs]
            sin_coarse = factor_ref[at + samples // FINE : at + samples // FINE + 1, fs]
            span = slice(a * FINE, (a + 1) * FINE)
            basis_ref[span, fs] = (cos_coarse * cos_fine + sin_coarse * sin_fine).astype(jnp.bfloat16)
            imag = sin_coarse * cos_fine - cos_coarse * sin_fine
            if f == 0:
                imag = jnp.where(lane == 0, alternate, imag)
            basis_ref[span, half_len + f * LANES : half_len + (f + 1) * LANES] = imag.astype(jnp.bfloat16)

    spectrum = jnp.dot(wave_ref[...], basis_ref[...], preferred_element_type=jnp.float32)
    spectrum = spectrum.astype(jnp.bfloat16).astype(jnp.float32)
    first = lax.broadcasted_iota(jnp.int32, (1, LANES), 1) == 0
    top = None
    for f in range(tiles):
        fs = slice(f * LANES, (f + 1) * LANES)
        real = spectrum[:, fs]
        imag = spectrum[:, half_len + f * LANES : half_len + (f + 1) * LANES]
        if f == 0:
            top = jnp.where(first, imag, 0.0).astype(jnp.bfloat16)
            imag = jnp.where(first, 0.0, imag)
        l1_ref[f] = real[:split]
        l2_ref[f] = real[:split] - imag[:split]
        l3_ref[f] = real[:split] + imag[:split]
        r1_ref[:, fs] = real[split:] + imag[split:]
        r2_ref[:, fs] = imag[split:]
        r3_ref[:, fs] = real[split:]
    highest = jnp.zeros((right, left), jnp.float32)
    for c in range(comps):
        highest += lax.dot_general(
            top[split + c * right : split + (c + 1) * right], top[c * left : (c + 1) * left],
            nt, preferred_element_type=jnp.float32,
        )

    def cross(index, even_out, odd_out):
        for f in range(tiles):
            fs = slice(f * LANES, (f + 1) * LANES)
            for u in range(chunk):
                i = index * chunk + u
                l1 = [l1_ref[f, pl.ds(c * left + i, 1), :] for c in range(comps)]
                l2 = [l2_ref[f, pl.ds(c * left + i, 1), :] for c in range(comps)]
                l3 = [l3_ref[f, pl.ds(c * left + i, 1), :] for c in range(comps)]
                for j in range(0, right, step):
                    k1 = r1_ref[j : j + step, fs] * l1[0]
                    k2 = r2_ref[j : j + step, fs] * l2[0]
                    k3 = r3_ref[j : j + step, fs] * l3[0]
                    for c in range(1, comps):
                        rows = slice(c * right + j, c * right + j + step)
                        k1 += r1_ref[rows, fs] * l1[c]
                        k2 += r2_ref[rows, fs] * l2[c]
                        k3 += r3_ref[rows, fs] * l3[c]
                    rows = slice(u * right + j, u * right + j + step)
                    even_out[rows, fs] = (k1 - k2).astype(jnp.bfloat16)
                    odd_out[rows, fs] = (k1 - k3).astype(jnp.bfloat16)

    column = lax.broadcasted_iota(jnp.int32, (1, left), 1)

    def lags(index, even_in, odd_in):
        even = jnp.dot(even_in[...], even_ref[...], preferred_element_type=jnp.float32)
        odd = jnp.dot(odd_in[...], odd_ref[...], preferred_element_type=jnp.float32)
        best = even + jnp.abs(odd)
        for u in range(chunk):
            here = column == index * chunk + u
            rows = best[u * right : (u + 1) * right]
            me_ref[...] = jnp.where(here, jnp.max(rows[:, :LANES], axis=1, keepdims=True), me_ref[...])
            mo_ref[...] = jnp.where(here, jnp.max(rows[:, LANES:], axis=1, keepdims=True), mo_ref[...])

    me_ref[...] = jnp.zeros_like(me_ref)
    mo_ref[...] = jnp.zeros_like(mo_ref)
    count = left // chunk
    cross(0, ce0, co0)
    copies[1].wait()
    copies[2].wait()

    def both(n, carry):
        cross(2 * n + 1, ce1, co1)
        lags(2 * n, ce0, co0)
        cross(jnp.minimum(2 * n + 2, count - 1), ce0, co0)
        lags(2 * n + 1, ce1, co1)
        return carry

    lax.fori_loop(0, count // 2, both, 0)

    alternating = highest.astype(jnp.bfloat16).astype(jnp.float32) / (2 * half_len)
    best = jnp.maximum(me_ref[...] + alternating, mo_ref[...] - alternating)
    best = jnp.maximum(best, earliest)
    wide = jnp.concatenate([best, jnp.zeros((right, LANES - left), jnp.float32)], axis=1)
    tall = jnp.concatenate([wide, jnp.zeros((LANES - right, LANES), jnp.float32)], axis=0)
    turned = tall.T
    owners, per_owner = out_ref.shape[0], left // out_ref.shape[0]
    for r in range(owners):
        out_ref[r, 0:per_owner, :] = turned[r * per_owner : (r + 1) * per_owner, :]


def similarity(left_waves, right_waves, comps, samples, owners):
    transform_len = samples + LAGS // 2
    half_len = transform_len // 2
    parts = samples // LANES
    left = left_waves.shape[0] // (comps * parts)
    right = right_waves.shape[0] // (comps * parts)
    tables = jnp.asarray(transform_tables(samples, transform_len, LAGS // 2))
    factors = 2 * (FINE + samples // FINE)
    chunk, step = 4, 32
    f32, bf16 = jnp.float32, jnp.bfloat16
    return pl.pallas_call(
        functools.partial(similarity_kernel, comps, samples, chunk, step),
        out_shape=jax.ShapeDtypeStruct((owners, 8, LANES), f32),
        in_specs=[pl.BlockSpec(memory_space=pltpu.VMEM)] * 2 + [pl.BlockSpec(memory_space=pltpu.HBM)],
        scratch_shapes=[
            pltpu.VMEM((3 * factors, half_len), bf16),
            pltpu.VMEM((factors, half_len), f32),
            pltpu.VMEM((samples, transform_len), bf16),
            *[pltpu.VMEM((half_len, LAGS // 2), bf16)] * 2,
            pltpu.VMEM((right * comps * parts, LANES), f32),
            pltpu.VMEM(((left + right) * comps, samples), bf16),
            *[pltpu.VMEM((half_len // LANES, left * comps, LANES), f32)] * 3,
            *[pltpu.VMEM((right * comps, half_len), f32)] * 3,
            *[pltpu.VMEM((chunk * right, half_len), bf16)] * 4,
            *[pltpu.VMEM((right, left), f32)] * 2,
            pltpu.SemaphoreType.DMA((3,)),
        ],
        compiler_params=pltpu.CompilerParams(vmem_limit_bytes=55_000_000),
        cost_estimate=pl.CostEstimate(flops=8_000_000_000, bytes_accessed=4_000_000, transcendentals=0),
        name="similarity",
    )(left_waves, right_waves, tables)


def assemble_kernel(width, in_ref, out_ref):
    for r in range(in_ref.shape[0]):
        out_ref[:, r * width : (r + 1) * width] = in_ref[r, 0 : out_ref.shape[0], 0:width]


def body(templates):
    per_device, comps, samples = templates.shape
    row_count = lax.axis_size("row")
    col_count = lax.axis_size("col")
    one, many = normalize(templates, col_count)
    partners = lax.all_to_all(many, "col", split_axis=0, concat_axis=0, tiled=True)
    owned = lax.all_gather(one, "row", tiled=True)
    partners = partners.reshape(col_count * one.shape[0], LANES)
    block = similarity(owned, partners, comps, samples, row_count)
    mine = lax.all_to_all(block, "row", split_axis=0, concat_axis=0, tiled=True)
    width = col_count * per_device
    return pl.pallas_call(
        functools.partial(assemble_kernel, width),
        out_shape=jax.ShapeDtypeStruct((per_device, row_count * width), jnp.float32),
        compiler_params=pltpu.CompilerParams(vmem_limit_bytes=4 << 20),
        name="assemble",
    )(mine)


def solution(mesh):
    placed = (P(("row", "col"), None, None),)
    return jax.shard_map(
        body, mesh=mesh, in_specs=placed, out_specs=P(("row", "col"), None), check_vma=False
    )
```

```python
import functools
import math

import jax
import jax.numpy as jnp
import numpy as np
from jax import lax
from jax.experimental import pallas as pl
from jax.experimental.pallas import tpu as pltpu
from jax.sharding import PartitionSpec as P

LAGS = 512
LANES = 128


FINE = 32


def lag_tables(transform_len, half_lags):
    half_len = transform_len // 2
    freq = np.arange(half_len)[:, None]
    lag = np.concatenate([np.arange(0, half_lags, 2), np.arange(1, half_lags, 2)])[None, :]
    angles = (freq * lag) % transform_len * (2.0 * math.pi / transform_len)
    weight = np.where(freq == 0, 1.0, 2.0) / transform_len
    sine = np.where(freq == 0, 0.0, -weight * np.sin(angles))
    both = np.concatenate([weight * np.cos(angles), sine], axis=1)
    return both.astype(np.float32).astype(jnp.bfloat16)


def normalize_kernel(copies, x_ref, one_ref, many_ref, rows_ref):
    per_device, comps, samples = x_ref.shape
    parts = samples // LANES
    for t in range(per_device):
        x = x_ref[t]
        scaling = lax.rsqrt(jnp.sum(x * x, axis=1, keepdims=True) / samples + 1e-06) / math.sqrt(samples)
        y = x * scaling
        for a in range(parts):
            rows_ref[pl.ds(t * comps * parts + a, comps, stride=parts), :] = y[:, a * LANES : (a + 1) * LANES]
    packed = rows_ref[...].astype(jnp.bfloat16)
    one_ref[...] = packed
    for q in range(copies):
        many_ref[q] = packed


def normalize(templates, copies):
    per_device, comps, samples = templates.shape
    rows = per_device * comps * samples // LANES
    return pl.pallas_call(
        functools.partial(normalize_kernel, copies),
        out_shape=(
            jax.ShapeDtypeStruct((rows, LANES), jnp.bfloat16),
            jax.ShapeDtypeStruct((copies, rows, LANES), jnp.bfloat16),
        ),
        scratch_shapes=[pltpu.VMEM((rows, LANES), jnp.float32)],
        compiler_params=pltpu.CompilerParams(vmem_limit_bytes=8 << 20),
        name="normalize",
    )(templates)


def similarity_kernel(comps, samples, chunk, step, *refs):
    (left_ref, right_ref, tables_hbm, out_ref,
     factor_ref, basis_ref, even_ref, odd_ref, rows_ref, wave_ref,
     l1_ref, l2_ref, l3_ref, r1_ref, r2_ref, r3_ref,
     ce0, co0, ce1, co1, me_ref, mo_ref, sems) = refs
    parts = samples // LANES
    left = left_ref.shape[0] // (comps * parts)
    right = right_ref.shape[0] // (comps * parts)
    half_len, lag_count = even_ref.shape
    tiles = half_len // LANES

    copies = [
        pltpu.make_async_copy(tables_hbm.at[:, :lag_count], even_ref, sems.at[0]),
        pltpu.make_async_copy(tables_hbm.at[:, lag_count:], odd_ref, sems.at[1]),
    ]
    for copy in copies:
        copy.start()

    def waves(src_ref, base, count):
        total = count * comps * parts
        rows_ref[0:total, :] = src_ref[...].astype(jnp.float32)
        for c in range(comps):
            for a in range(parts):
                wave_ref[base + c * count : base + (c + 1) * count, a * LANES : (a + 1) * LANES] = rows_ref[
                    pl.ds(c * parts + a, count, stride=comps * parts), :
                ].astype(jnp.bfloat16)

    split = comps * left
    waves(left_ref, 0, left)
    waves(right_ref, split, right)

    nt = (((1,), (1,)), ((), ()))
    shift = LAGS // 2
    earliest = jnp.zeros((right, left), jnp.float32)
    for c in range(comps):
        earliest += lax.dot_general(
            wave_ref[split + c * right : split + (c + 1) * right, : samples - shift],
            wave_ref[c * left : (c + 1) * left, shift:],
            nt, preferred_element_type=jnp.float32,
        )

    coarse_count = samples // FINE
    for f in range(tiles):
        fs = slice(f * LANES, (f + 1) * LANES)
        for base, count, stride in ((0, FINE, 1), (2 * FINE, coarse_count, FINE)):
            multiple = lax.broadcasted_iota(jnp.int32, (count, LANES), 0) * stride
            freq = lax.broadcasted_iota(jnp.int32, (count, LANES), 1) + f * LANES
            angle = lax.rem(multiple * freq, 2 * half_len).astype(jnp.float32) * (math.pi / half_len)
            factor_ref[base : base + count, fs] = jnp.cos(angle)
            sine = jnp.sin(angle)
            factor_ref[base + count : base + 2 * count, fs] = -sine if stride > 1 else sine
    lane = lax.broadcasted_iota(jnp.int32, (FINE, LANES), 1)
    row = lax.broadcasted_iota(jnp.int32, (FINE, LANES), 0)
    alternate = jnp.where(lax.rem(row, 2) == 0, 1.0, -1.0)
    first = lax.broadcasted_iota(jnp.int32, (1, LANES), 1) == 0

    def make_basis(f):
        fs = slice(f * LANES, (f + 1) * LANES)
        cos_fine, sin_fine = factor_ref[:FINE, fs], factor_ref[FINE : 2 * FINE, fs]
        for a in range(samples // FINE):
            at = 2 * FINE + a
            cos_coarse = factor_ref[at : at + 1, fs]
            sin_coarse = factor_ref[at + samples // FINE : at + samples // FINE + 1, fs]
            span = slice(a * FINE, (a + 1) * FINE)
            basis_ref[f, span, :LANES] = (cos_coarse * cos_fine + sin_coarse * sin_fine).astype(jnp.bfloat16)
            imag = sin_coarse * cos_fine - cos_coarse * sin_fine
            if f == 0:
                imag = jnp.where(lane == 0, alternate, imag)
            basis_ref[f, span, LANES:] = imag.astype(jnp.bfloat16)

    def transform(f):
        fs = slice(f * LANES, (f + 1) * LANES)
        spectrum = jnp.dot(wave_ref[...], basis_ref[f], preferred_element_type=jnp.float32)
        spectrum = spectrum.astype(jnp.bfloat16).astype(jnp.float32)
        real, imag = spectrum[:, :LANES], spectrum[:, LANES:]
        top = None
        if f == 0:
            top = jnp.where(first, imag, 0.0).astype(jnp.bfloat16)
            imag = jnp.where(first, 0.0, imag)
        l1_ref[f] = real[:split]
        l2_ref[f] = real[:split] - imag[:split]
        l3_ref[f] = real[:split] + imag[:split]
        r1_ref[:, fs] = real[split:] + imag[split:]
        r2_ref[:, fs] = imag[split:]
        r3_ref[:, fs] = real[split:]
        return top

    make_basis(0)
    tops = []
    for f in range(tiles):
        if f + 1 < tiles:
            make_basis(f + 1)
        tops.append(transform(f))
    top = tops[0]
    highest = jnp.zeros((right, left), jnp.float32)
    for c in range(comps):
        highest += lax.dot_general(
            top[split + c * right : split + (c + 1) * right], top[c * left : (c + 1) * left],
            nt, preferred_element_type=jnp.float32,
        )

    def cross(index, even_out, odd_out):
        for f in range(tiles):
            fs = slice(f * LANES, (f + 1) * LANES)
            for u in range(chunk):
                i = index * chunk + u
                l1 = [l1_ref[f, pl.ds(c * left + i, 1), :] for c in range(comps)]
                l2 = [l2_ref[f, pl.ds(c * left + i, 1), :] for c in range(comps)]
                l3 = [l3_ref[f, pl.ds(c * left + i, 1), :] for c in range(comps)]
                for j in range(0, right, step):
                    k1 = r1_ref[j : j + step, fs] * l1[0]
                    k2 = r2_ref[j : j + step, fs] * l2[0]
                    k3 = r3_ref[j : j + step, fs] * l3[0]
                    for c in range(1, comps):
                        rows = slice(c * right + j, c * right + j + step)
                        k1 += r1_ref[rows, fs] * l1[c]
                        k2 += r2_ref[rows, fs] * l2[c]
                        k3 += r3_ref[rows, fs] * l3[c]
                    rows = slice(u * right + j, u * right + j + step)
                    even_out[rows, fs] = (k1 - k2).astype(jnp.bfloat16)
                    odd_out[rows, fs] = (k1 - k3).astype(jnp.bfloat16)

    column = lax.broadcasted_iota(jnp.int32, (1, left), 1)

    def lags(index, even_in, odd_in):
        even = jnp.dot(even_in[...], even_ref[...], preferred_element_type=jnp.float32)
        odd = jnp.dot(odd_in[...], odd_ref[...], preferred_element_type=jnp.float32)
        best = even + jnp.abs(odd)
        for u in range(chunk):
            here = column == index * chunk + u
            rows = best[u * right : (u + 1) * right]
            me_ref[...] = jnp.where(here, jnp.max(rows[:, :LANES], axis=1, keepdims=True), me_ref[...])
            mo_ref[...] = jnp.where(here, jnp.max(rows[:, LANES:], axis=1, keepdims=True), mo_ref[...])

    me_ref[...] = jnp.zeros_like(me_ref)
    mo_ref[...] = jnp.zeros_like(mo_ref)
    count = left // chunk
    cross(0, ce0, co0)
    for copy in copies:
        copy.wait()

    def both(n, carry):
        cross(2 * n + 1, ce1, co1)
        lags(2 * n, ce0, co0)
        cross(2 * n + 2, ce0, co0)
        lags(2 * n + 1, ce1, co1)
        return carry

    lax.fori_loop(0, count // 2 - 1, both, 0)
    cross(count - 1, ce1, co1)
    lags(count - 2, ce0, co0)
    lags(count - 1, ce1, co1)

    alternating = highest.astype(jnp.bfloat16).astype(jnp.float32) / (2 * half_len)
    best = jnp.maximum(me_ref[...] + alternating, mo_ref[...] - alternating)
    best = jnp.maximum(best, earliest)
    wide = jnp.concatenate([best, jnp.zeros((right, LANES - left), jnp.float32)], axis=1)
    tall = jnp.concatenate([wide, jnp.zeros((LANES - right, LANES), jnp.float32)], axis=0)
    turned = tall.T
    owners, per_owner = out_ref.shape[0], left // out_ref.shape[0]
    for r in range(owners):
        out_ref[r, 0:per_owner, :] = turned[r * per_owner : (r + 1) * per_owner, :]


def similarity(left_waves, right_waves, comps, samples, owners):
    transform_len = samples + LAGS // 2
    half_len = transform_len // 2
    parts = samples // LANES
    left = left_waves.shape[0] // (comps * parts)
    right = right_waves.shape[0] // (comps * parts)
    tables = jnp.asarray(lag_tables(transform_len, LAGS // 2))
    factors = 2 * (FINE + samples // FINE)
    chunk, step = 8, 32
    f32, bf16 = jnp.float32, jnp.bfloat16
    return pl.pallas_call(
        functools.partial(similarity_kernel, comps, samples, chunk, step),
        out_shape=jax.ShapeDtypeStruct((owners, 8, LANES), f32),
        in_specs=[pl.BlockSpec(memory_space=pltpu.VMEM)] * 2 + [pl.BlockSpec(memory_space=pltpu.HBM)],
        scratch_shapes=[
            pltpu.VMEM((factors, half_len), f32),
            pltpu.VMEM((half_len // LANES, samples, 2 * LANES), bf16),
            *[pltpu.VMEM((half_len, LAGS // 2), bf16)] * 2,
            pltpu.VMEM((right * comps * parts, LANES), f32),
            pltpu.VMEM(((left + right) * comps, samples), bf16),
            *[pltpu.VMEM((half_len // LANES, left * comps, LANES), f32)] * 3,
            *[pltpu.VMEM((right * comps, half_len), f32)] * 3,
            *[pltpu.VMEM((chunk * right, half_len), bf16)] * 4,
            *[pltpu.VMEM((right, left), f32)] * 2,
            pltpu.SemaphoreType.DMA((2,)),
        ],
        compiler_params=pltpu.CompilerParams(vmem_limit_bytes=55_300_000),
        cost_estimate=pl.CostEstimate(flops=8_000_000_000, bytes_accessed=4_000_000, transcendentals=0),
        name="similarity",
    )(left_waves, right_waves, tables)


def assemble_kernel(width, in_ref, out_ref):
    for r in range(in_ref.shape[0]):
        out_ref[:, r * width : (r + 1) * width] = in_ref[r, 0 : out_ref.shape[0], 0:width]


def body(templates):
    per_device, comps, samples = templates.shape
    row_count = lax.axis_size("row")
    col_count = lax.axis_size("col")
    one, many = normalize(templates, col_count)
    partners = lax.all_to_all(many, "col", split_axis=0, concat_axis=0, tiled=True)
    owned = lax.all_gather(one, "row", tiled=True)
    partners = partners.reshape(col_count * one.shape[0], LANES)
    block = similarity(owned, partners, comps, samples, row_count)
    mine = lax.all_to_all(block, "row", split_axis=0, concat_axis=0, tiled=True)
    width = col_count * per_device
    return pl.pallas_call(
        functools.partial(assemble_kernel, width),
        out_shape=jax.ShapeDtypeStruct((per_device, row_count * width), jnp.float32),
        compiler_params=pltpu.CompilerParams(vmem_limit_bytes=4 << 20),
        name="assemble",
    )(mine)


def solution(mesh):
    placed = (P(("row", "col"), None, None),)
    return jax.shard_map(
        body, mesh=mesh, in_specs=placed, out_specs=P(("row", "col"), None), check_vma=False
    )
```
